512 devices in a mesh: virt: 32 (over x, z), aux: 16 (over y, core).
Axes of the slice: x: 4, y: 8, z: 8, core: 2. Of those that a mesh axis runs over, the one named last changes fastest.
Arguments:
- three_index: bfloat16 [2400, 20480], P('aux', 'virt'), may hold values from -0.0625 to 0.0625
- eps_occ: float32 [20], replicated, may hold values from -1.5 to -0.5
- eps_virt: float32 [1024], replicated, may hold values from 0.3 to 3
Outputs:
- virt_energy: float32 [1024], P('virt')
- pair_energy: float32 [20, 20], replicated
The draws below stay inside these ranges and needn't reach their ends.
All inputs are finite; a program needn't handle non-finite values.
Results may differ from the reference program's by a relative error of at most 0.0003.
Values may be sent and summed in bfloat16 or wider, within the bound.
No kernel may reach another device: no remote copies, remote signals or barrier semaphores. Data moves between devices by JAX's collectives and lax.ppermute only.
A program may use at most 128 MiB of HBM per device.

```python
import jax
import jax.numpy as jnp
from jax import lax

O = 20
VIRT_DEV = 32
VIRT = 1024
AUX = 2400


def level_of(own_key, shape, split, low, largest):
    gain = 1.0
    for axis_at, blocks in split:
        steps = jax.random.uniform(jax.random.fold_in(jax.random.fold_in(own_key, 6), axis_at), (blocks,), jnp.float32, low / len(split), largest / len(split))
        gain = gain * jnp.repeat(jnp.exp(steps), shape[axis_at] // blocks).reshape((-1,) + (1,) * (len(shape) - 1 - axis_at))
    return gain


def scatter_about(key, dims, spread, limit, split=(), kind=jnp.bfloat16):
    result = jax.random.normal(key, dims, jnp.float32) * spread
    if len(split) > 0:
        result = level_of(key, dims, split, -0.22, 0.18) * result
    return jnp.clip(result, min=-limit, max=limit).astype(kind)


def setup_inputs(seed: int = 0) -> dict:
    splits = jax.random.split(jax.random.key(seed), 4)
    three_index = scatter_about(splits[0], (AUX, VIRT * O), 0.011, 0.0625, ((0, 16), (1, 32)))
    eps_occ = jnp.clip(jax.random.uniform(splits[1], (O,), jnp.float32, -1.5, -0.5), -1.5, -0.5)
    eps_virt = jnp.clip(jax.random.uniform(splits[2], (VIRT,), jnp.float32, 0.3, 3.0), 0.3, 3.0)
    return {"three_index": three_index, "eps_occ": eps_occ, "eps_virt": eps_virt}


def reference(three_index, eps_occ, eps_virt):
    block_count = VIRT // VIRT_DEV
    widened = three_index.astype(jnp.float32).reshape(AUX, VIRT, O)

    def one_block(which):
        offset = (which * VIRT_DEV).astype(jnp.int32)
        left_rows = lax.dynamic_slice_in_dim(widened, offset, VIRT_DEV, 1)
        integrals = jnp.einsum("pai,pbj->iajb", left_rows, widened, precision=lax.Precision.HIGHEST)
        eps_own = lax.dynamic_slice_in_dim(eps_virt, offset, VIRT_DEV)
        denominator = (eps_occ[:, None, None, None] + eps_occ[None, None, :, None]
                       - eps_own[None, :, None, None] - eps_virt[None, None, None, :])
        swapped = jnp.transpose(integrals, (2, 1, 0, 3))
        energy_terms = integrals * (2.0 * integrals - swapped) / denominator
        return jnp.sum(energy_terms, axis=(0, 2, 3)), jnp.sum(energy_terms, axis=(1, 3))

    virt_parts, pair_parts = lax.map(one_block, jnp.arange(block_count, dtype=jnp.int32))
    return virt_parts.reshape(VIRT), jnp.sum(pair_parts, axis=0)
```

```python
import functools

import jax
import jax.numpy as jnp
from jax import lax
from jax.experimental import pallas as pl
from jax.experimental.pallas import tpu as pltpu
from jax.sharding import Mesh
from jax.sharding import PartitionSpec as P

SWAP = [(0, 1), (1, 0)]
LANES = 128


def ring_by_core(n):
    pairs = []
    for k in range(n):
        pairs.append((2 * k, 2 * ((k - 1) % n)))
        pairs.append((2 * k + 1, 2 * ((k + 1) % n) + 1))
    return pairs


def prepare(x_ref, own_ref, *, occ, own):
    width = occ * own
    rows = x_ref.shape[0]
    source = lax.broadcasted_iota(jnp.int32, (width, width), 0)
    target = lax.broadcasted_iota(jnp.int32, (width, width), 1)
    hot = ((target % own) * occ + target // own == source).astype(jnp.bfloat16)
    moved = jnp.dot(x_ref[...], hot, preferred_element_type=jnp.float32)
    own_ref[...] = jnp.zeros_like(own_ref)
    own_ref[pl.ds(0, rows), :] = moved.astype(jnp.bfloat16)


def joined(order_ref, tiles_ref, out_ref):
    count, _, part = tiles_ref.shape
    for k in range(count):
        out_ref[:, k * part : (k + 1) * part] = tiles_ref[order_ref[k]]


def transposed_groups(tiles, lane):
    a, b, c, d = tiles
    low = lane < 64
    a, c = jnp.where(low, a, pltpu.roll(c, 64, 1)), jnp.where(low, pltpu.roll(a, 64, 1), c)
    b, d = jnp.where(low, b, pltpu.roll(d, 64, 1)), jnp.where(low, pltpu.roll(b, 64, 1), d)
    even = (lane // 32) % 2 == 0
    a, b = jnp.where(even, a, pltpu.roll(b, 32, 1)), jnp.where(even, pltpu.roll(a, 96, 1), b)
    c, d = jnp.where(even, c, pltpu.roll(d, 32, 1)), jnp.where(even, pltpu.roll(c, 96, 1), d)
    return a, b, c, d


def energies(eps_ref, left_ref, b0_ref, b1_ref, la_ref, vb_ref, sum_ref, share_ref, c_ref, *, occ):
    half = b0_ref.shape[0]
    for at, b_ref in ((0, b0_ref), (half, b1_ref)):
        found = jnp.dot(b_ref[...], left_ref[...], preferred_element_type=jnp.float32)
        for t in range(c_ref.shape[0]):
            c_ref[t, pl.ds(at, half), :] = found[:, t * LANES : (t + 1) * LANES]
    lane = lax.broadcasted_iota(jnp.int32, (8, LANES), 1)
    groups = occ // 4
    vb = vb_ref[...]

    def tile(j, t):
        return c_ref[t, pl.ds(j, 8, stride=occ), :]

    share = jnp.zeros((8, LANES), jnp.float32)
    for tj in range(groups):
        for ti in range(groups):
            other = transposed_groups([tile(4 * ti + g, tj) for g in range(4)], lane)
            la = la_ref[:, ti * LANES : (ti + 1) * LANES] - vb
            for g in range(4):
                j = 4 * tj + g
                m = tile(j, ti)
                e = m * (2.0 * m - other[g]) / (la + eps_ref[j])
                share = share + e
                sum_ref[j : j + 1, ti * LANES : (ti + 1) * LANES] = jnp.sum(e, axis=0, keepdims=True)
    share_ref[...] = share


def on_device(three_index, eps_occ, eps_virt):
    occ = eps_occ.shape[0]
    rows, width = three_index.shape
    own = width // occ
    nx, nz, ny = lax.axis_size("x"), lax.axis_size("z"), lax.axis_size("y")
    parts = 2 * ny
    x, z, y, c = (lax.axis_index(k) for k in ("x", "z", "y", "c"))
    few = own // parts
    cols = few * occ
    part = -(-rows // 8) * 8
    vmem = pl.BlockSpec(memory_space=pltpu.VMEM)
    smem = pl.BlockSpec(memory_space=pltpu.SMEM)

    turned = jnp.pad(three_index, ((0, part - rows), (0, 0))).T.reshape(parts, cols, part)
    tiles = lax.all_to_all(turned, ("y", "c"), split_axis=0, concat_axis=0, tiled=True)
    sign = 1 - 2 * c
    order = [2 * y + c, 2 * y + 1 - c]
    for k in range(1, ny // 2 + 1):
        at = 2 * ((y + sign * k) % ny)
        order += [at + c, at + 1 - c]
    for k in range(1, ny // 2):
        at = 2 * ((y - sign * k) % ny)
        order += [at + 1 - c, at + c]
    order = jnp.stack(order).astype(jnp.int32)
    unit = pl.pallas_call(
        joined,
        out_shape=jax.ShapeDtypeStruct((cols, parts * part), jnp.bfloat16),
        in_specs=[smem, vmem],
        out_specs=vmem,
    )(order, tiles)

    mine = pl.pallas_call(
        functools.partial(prepare, occ=occ, own=own),
        out_shape=jax.ShapeDtypeStruct((part, width), jnp.bfloat16),
        in_specs=[vmem],
        out_specs=vmem,
    )(three_index)
    both = jnp.stack([mine, lax.ppermute(mine, "c", SWAP)])
    arrived, moving = [], both
    for _ in range(ny // 2):
        moving = lax.ppermute(moving, ("y", "c"), ring_by_core(ny))
        arrived.append(moving)
    swapped = lax.ppermute(jnp.stack(arrived[:-1]), "c", SWAP)
    left = jnp.concatenate([both, *arrived, swapped.reshape(-1, part, width)]).reshape(-1, width)

    near, far = (lax.ppermute(unit, "x", [(k, (k - d) % nx) for k in range(nx)]) for d in (1, 2))
    up, down = jnp.concatenate([unit, near]), jnp.concatenate([near, far])
    steps = nz // 2
    table = jnp.tile(eps_virt.reshape(nx, nz, parts, few), (2, 2, 1, 1))
    table = lax.dynamic_slice(table, (x, z, 2 * y + c, 0), (nx, nz, 1, few)).reshape(nx, nz, few)
    vb = [jnp.concatenate([table[0:2, k], table[1:3, -k % nz]]) for k in range(steps + 1)]
    vb = jnp.broadcast_to(jnp.stack(vb).reshape(steps + 1, 4 * few, 1), (steps + 1, 4 * few, LANES))
    eps_own = lax.dynamic_slice_in_dim(eps_virt, (x * nz + z) * own, own)
    la = jnp.broadcast_to((eps_occ[:, None] - eps_own[None, :]).reshape(1, width), (8, width))
    total, spread = None, jnp.zeros((nx, nz, few), jnp.float32)
    call = pl.pallas_call(
        functools.partial(energies, occ=occ),
        out_shape=[jax.ShapeDtypeStruct((occ, width), jnp.float32), jax.ShapeDtypeStruct((8, LANES), jnp.float32)],
        in_specs=[smem] + [vmem] * 5,
        out_specs=[vmem] * 2,
        scratch_shapes=[pltpu.VMEM((width // LANES, 4 * cols, LANES), jnp.float32)],
        cost_estimate=pl.CostEstimate(flops=8 * cols * width * parts * part, bytes_accessed=4 << 20, transcendentals=0),
    )
    for k in range(steps + 1):
        if k:
            up = lax.ppermute(up, "z", [(n, (n - 1) % nz) for n in range(nz)])
            down = lax.ppermute(down, "z", [(n, (n + 1) % nz) for n in range(nz)])
        part_sum, share = call(eps_occ, left, up, down, la, vb[k])
        weight = 0.5 if k in (0, steps) else 1.0
        part_sum = part_sum * weight
        total = part_sum if total is None else total + part_sum
        share = (jnp.sum(share, axis=1) * weight).reshape(2, 2, few)
        spread = spread.at[0:2, k].add(share[0]).at[1:3, -k % nz].add(share[1])

    cube = total.reshape(occ, occ, own)
    pairs = jnp.sum(cube, axis=2).reshape(-1)
    left_share = jnp.sum(cube, axis=(0, 1))
    wide = jnp.zeros((2 * nx, 2 * nz, own), jnp.float32)
    wide = lax.dynamic_update_slice(wide, left_share.reshape(1, 1, own), (x, z, 0)) + lax.dynamic_update_slice(
        wide, spread, (x, z, few * (2 * y + c))
    )
    spread = jnp.sum(wide.reshape(2, nx, 2, nz, own), axis=(0, 2))

    first = jnp.concatenate([spread.reshape(nx, nz * own), jnp.broadcast_to(pairs, (nx, occ * occ))], axis=1)
    first = jnp.broadcast_to(first[:, None, :], (nx, parts, first.shape[1])).reshape(nx * parts, -1)
    first = jnp.sum(lax.all_to_all(first, ("x", "y", "c"), split_axis=0, concat_axis=0, tiled=True), axis=0)
    second = jnp.concatenate(
        [first[: nz * own].reshape(nz, own), jnp.broadcast_to(first[nz * own :], (nz, occ * occ))], axis=1
    )
    second = jnp.sum(lax.all_to_all(second, "z", split_axis=0, concat_axis=0, tiled=True), axis=0)
    square = second[own:].reshape(occ, occ)
    return second[:own], square + square.T


def solution(mesh):
    split = Mesh(mesh.devices.reshape(4, 8, mesh.shape["aux"] // 2, 2), ("x", "z", "y", "c"))
    placed = (P(("y", "c"), ("x", "z")), P(), P())
    return jax.shard_map(
        on_device, mesh=split, in_specs=placed, out_specs=(P(("x", "z")), P()), check_vma=False
    )
```

```python
import functools

import jax
import jax.numpy as jnp
from jax import lax
from jax.experimental import pallas as pl
from jax.experimental.pallas import tpu as pltpu
from jax.sharding import Mesh
from jax.sharding import PartitionSpec as P


SWAP = [(0, 1), (1, 0)]
LANES = 128
BF, F32 = jnp.bfloat16, jnp.float32
HIGH = lax.Precision.HIGHEST
VMEM = pl.BlockSpec(memory_space=pltpu.VMEM)
SMEM = pl.BlockSpec(memory_space=pltpu.SMEM)


def iota(shape, dim):
    return lax.broadcasted_iota(jnp.int32, shape, dim)


def ring_by_core(n):
    pairs = []
    for k in range(n):
        pairs.append((2 * k, 2 * ((k - 1) % n)))
        pairs.append((2 * k + 1, 2 * ((k + 1) % n) + 1))
    return pairs


def turn(x_ref, out_ref):
    rows, width = x_ref.shape
    same = (iota((LANES, LANES), 0) == iota((LANES, LANES), 1)).astype(BF)
    out_ref[...] = jnp.zeros_like(out_ref)
    for at in range(0, width, LANES):
        block = x_ref[:, at : at + LANES]
        turned = lax.dot_general(same, block, (((1,), (1,)), ((), ())), preferred_element_type=F32)
        out_ref[at : at + LANES, 0:rows] = turned.astype(BF)


def prepare(x_ref, own_ref, *, occ, own):
    width = occ * own
    rows = x_ref.shape[0]
    target = iota((1, width), 1)
    source = lax.rem(target, own) * occ + lax.div(target, own)
    hot = (iota((width, width), 0) == source).astype(BF)
    moved = jnp.dot(x_ref[...], hot, preferred_element_type=F32)
    own_ref[...] = jnp.zeros_like(own_ref)
    own_ref[pl.ds(0, rows), :] = moved.astype(BF)


def joined(at_ref, own_ref, other_ref, out_ref, *, part):
    ny = own_ref.shape[0]
    y, c = at_ref[2], at_ref[3]
    for k in range(ny):
        step = k if k <= ny // 2 else ny // 2 - k
        near, far = (own_ref, other_ref) if step >= 0 else (other_ref, own_ref)
        source = lax.rem(y + ny + (1 - 2 * c) * step, ny)
        at = 2 * k * part
        out_ref[:, at : at + part] = near[source, :, 0:part]
        out_ref[:, at + part : at + 2 * part] = far[source, :, 0:part]


def stack(pieces, out_ref):
    at = 0
    for piece in pieces:
        for k in range(piece.shape[0]):
            out_ref[at : at + piece.shape[1], :] = piece[k]
            at += piece.shape[1]


def transposed_groups(tiles, lane):
    a, b, c, d = tiles
    low = lane < 64
    a, c = jnp.where(low, a, pltpu.roll(c, 64, 1)), jnp.where(low, pltpu.roll(a, 64, 1), c)
    b, d = jnp.where(low, b, pltpu.roll(d, 64, 1)), jnp.where(low, pltpu.roll(b, 64, 1), d)
    even = (lane // 32) % 2 == 0
    a, b = jnp.where(even, a, pltpu.roll(b, 32, 1)), jnp.where(even, pltpu.roll(a, 96, 1), b)
    c, d = jnp.where(even, c, pltpu.roll(d, 32, 1)), jnp.where(even, pltpu.roll(c, 96, 1), d)
    return a, b, c, d


def energies(at_ref, eps_ref, virt_ref, b0_ref, b1_ref, *refs, occ, own, nx, nz, few, k, weight, pieces):
    *refs, c_ref, b_ref = refs
    if pieces:
        left_ref, sum_ref, share_ref = refs[pieces:]
        stack(refs[:pieces], left_ref)
    else:
        left_ref, before_ref, sum_ref, share_ref = refs
    half = b0_ref.shape[0]
    b_ref[pl.ds(0, half), :] = b0_ref[...]
    b_ref[pl.ds(half, half), :] = b1_ref[...]
    found = jnp.dot(b_ref[...], left_ref[...], preferred_element_type=F32)
    for t in range(c_ref.shape[0]):
        c_ref[t] = found[:, t * LANES : (t + 1) * LANES]
    lane, row = iota((8, LANES), 1), iota((8, LANES), 0)
    x, z, y, c = (at_ref[n] for n in range(4))
    vb = jnp.zeros((8, LANES), F32)
    for r in range(8):
        unit = r // few
        beside = jnp.where(c == 0, 2 * unit, 3 - 2 * unit)
        there = lax.rem(x + beside, nx) * nz + lax.rem(z + jnp.where(c == 0, k, nz - k), nz)
        vb = jnp.where(row == r, virt_ref[there * own + y * few + r % few], vb)
    va = jnp.zeros((8, LANES), F32)
    for a in range(own):
        va = jnp.where(lax.rem(lane, own) == a, virt_ref[(x * nz + z) * own + a], va)
    va = va + vb
    groups = occ // 4

    def tile(j, t):
        return c_ref[t, pl.ds(j, 8, stride=occ), :]

    share = jnp.zeros((8, LANES), F32)
    for ti in range(groups):
        la = -va
        for g in range(4):
            la = jnp.where(lax.div(lane, own) == g, eps_ref[4 * ti + g] - va, la)
        at = slice(ti * LANES, (ti + 1) * LANES)
        for tj in range(groups):
            other = transposed_groups([tile(4 * ti + g, tj) for g in range(4)], lane)
            for g in range(4):
                j = 4 * tj + g
                m = tile(j, ti)
                e = m * (2.0 * m - other[g]) / (la + eps_ref[j])
                if weight != 1.0:
                    e = e * weight
                share = share + e
                total = jnp.sum(e, axis=0, keepdims=True)
                sum_ref[j : j + 1, at] = total if pieces else total + before_ref[j : j + 1, at]
    share_ref[...] = share


def finish(at_ref, total_ref, *refs, occ, own, nx, nz, few):
    *share_refs, out_ref = refs
    width = total_ref.shape[1]
    x, z, y, c = (at_ref[n] for n in range(4))
    wide, spots = 4 * LANES, nz * own
    total = total_ref[...]
    hot = (iota((width, wide), 1) % occ == iota((width, wide), 0) // own).astype(F32)
    pairs = jnp.dot(total, hot, preferred_element_type=F32, precision=HIGH)
    pairs = jnp.where(iota((occ, wide), 1) // occ == iota((occ, wide), 0), pairs, 0.0)
    pairs = jnp.sum(pairs, axis=0, keepdims=True)
    spot = iota((width, spots), 1)
    hot = ((spot // own == z) & (spot % own == iota((width, spots), 0) % own)).astype(F32)
    left = jnp.dot(jnp.sum(total, axis=0, keepdims=True), hot, preferred_element_type=F32, precision=HIGH)
    row, spot = iota((8, spots), 0), iota((8, spots), 1)
    kept = jnp.zeros((8, spots), F32)
    for k, ref in enumerate(share_refs):
        share = jnp.sum(ref[...], axis=1, keepdims=True)
        goal = lax.rem(z + jnp.where(c == 0, k, nz - k), nz) * own + y * few + lax.rem(row, few)
        kept = kept + jnp.where(spot == goal, share, 0.0)
    unit = lax.div(row[:, 0:1], few)
    shift = jnp.where(c == 0, 2 * unit, 3 - 2 * unit)
    each = out_ref.shape[0] // nx
    for there in range(nx):
        mine = jnp.sum(jnp.where(lax.rem(x + shift, nx) == there, kept, 0.0), axis=0, keepdims=True)
        mine = mine + jnp.where(x == there, left, 0.0)
        for k in range(there * each, (there + 1) * each):
            out_ref[k, :, 0:spots] = mine
            out_ref[k, :, spots : spots + wide] = pairs


def middle(in_ref, out_ref, *, own):
    got = jnp.sum(in_ref[...], axis=0)
    nz = out_ref.shape[0]
    spots = nz * own
    for k in range(nz):
        base = (k * own) // LANES * LANES
        piece = got[:, base : base + LANES]
        turned = (LANES - (k * own - base)) % LANES
        out_ref[k, :, 0:LANES] = pltpu.roll(piece, turned, 1) if turned else piece
        out_ref[k, :, LANES:] = got[:, spots:]


def last(in_ref, virt_ref, pair_ref, *, occ, own):
    got = jnp.sum(in_ref[...], axis=0)
    virt_ref[...] = got[:, 0:own]
    row = got[:, LANES:]
    wide = row.shape[1]
    n, j = iota((occ, wide), 1), iota((occ, wide), 0)
    m, i = iota((wide, occ), 0), iota((wide, occ), 1)
    one = jnp.dot(jnp.where(n // occ == j, row, 0.0), (m % occ == i).astype(F32), preferred_element_type=F32, precision=HIGH)
    two = jnp.dot(jnp.where(n % occ == j, jnp.where(n < occ * occ, row, 0.0), 0.0), (m // occ == i).astype(F32), preferred_element_type=F32, precision=HIGH)
    pair_ref[...] = one + two


def shape(*dims, kind=F32):
    return jax.ShapeDtypeStruct(dims, kind)


def on_device(three_index, eps_occ, eps_virt):
    occ = eps_occ.shape[0]
    rows, width = three_index.shape
    own = width // occ
    nx, nz, ny = lax.axis_size("x"), lax.axis_size("z"), lax.axis_size("y")
    parts = 2 * ny
    x, z, y, c = (lax.axis_index(k) for k in ("x", "z", "y", "c"))
    few = own // ny
    cols = few * occ
    part = -(-rows // 8) * 8
    steps = nz // 2
    place = jnp.stack([x, z, y, c]).astype(jnp.int32)

    def kernel(f, out, spaces, cost=0, scratch=(), **static):
        several = isinstance(out, list)
        return pl.pallas_call(
            functools.partial(f, **static),
            out_shape=out,
            in_specs=spaces,
            out_specs=[VMEM] * len(out) if several else VMEM,
            scratch_shapes=scratch,
            compiler_params=pltpu.CompilerParams(vmem_limit_bytes=16 << 20),
            cost_estimate=pl.CostEstimate(flops=cost, bytes_accessed=1 << 20, transcendentals=0),
        )

    turned = kernel(turn, shape(width, 2 * LANES, kind=BF), [VMEM])(three_index).reshape(ny, cols, -1)
    tiles = lax.all_to_all(turned, "y", split_axis=0, concat_axis=0, tiled=True)
    theirs = lax.ppermute(tiles, "c", SWAP)
    unit = kernel(joined, shape(cols, parts * part, kind=BF), [SMEM] + [VMEM] * 2, part=part)(place, tiles, theirs)

    mine = kernel(prepare, shape(part, width, kind=BF), [VMEM], occ=occ, own=own)(three_index)
    both = jnp.stack([mine, lax.ppermute(mine, "c", SWAP)])
    arrived, moving = [], both
    for _ in range(ny // 2):
        moving = lax.ppermute(moving, ("y", "c"), ring_by_core(ny))
        arrived.append(moving)
    collected = jnp.concatenate(arrived[:-1])
    outer = lax.ppermute(collected, "c", SWAP)

    def beside(n):
        return [(2 * m + core, 2 * ((m - 2 * n + core * (4 * n - 3)) % nx) + core) for m in range(nx) for core in range(2)]

    one, two = (lax.ppermute(unit, ("x", "c"), beside(n)) for n in range(2))
    total, shares = None, []
    for k in range(steps + 1):
        if k:
            one = lax.ppermute(one, ("z", "c"), ring_by_core(nz))
            two = lax.ppermute(two, ("z", "c"), ring_by_core(nz))
        given = (left, total) if k else (both, *arrived, outer)
        sizes = [shape(occ, width), shape(8, LANES)]
        call = kernel(
            energies,
            sizes if k else [shape(parts * part, width, kind=BF), *sizes],
            [SMEM] * 3 + [VMEM] * (2 + len(given)),
            cost=4 * cols * width * parts * part,
            scratch=[
                pltpu.VMEM((width // LANES, 2 * cols, LANES), F32),
                pltpu.VMEM((2 * cols, parts * part), BF),
            ],
            occ=occ, own=own, nx=nx, nz=nz, few=few, k=k,
            weight=0.5 if k in (0, steps) else 1.0,
            pieces=0 if k else len(given),
        )
        results = call(place, eps_occ, eps_virt, one, two, *given)
        if k == 0:
            left, *results = results
        total, share = results
        shares.append(share)

    wide = nz * own + 4 * LANES
    slots = kernel(
        finish, shape(nx * parts, 1, wide), [SMEM] + [VMEM] * (2 + steps), occ=occ, own=own, nx=nx, nz=nz, few=few
    )(place, total, *shares)
    slots = lax.all_to_all(slots, ("x", "y", "c"), split_axis=0, concat_axis=0, tiled=True)
    slots = kernel(middle, shape(nz, 1, 5 * LANES), [VMEM], own=own)(slots)
    slots = lax.all_to_all(slots, "z", split_axis=0, concat_axis=0, tiled=True)
    virt, pairs = kernel(last, [shape(1, own), shape(occ, occ)], [VMEM], occ=occ, own=own)(slots)
    return virt.reshape(own), pairs


def solution(mesh):
    split = Mesh(mesh.devices.reshape(4, 8, mesh.shape["aux"] // 2, 2), ("x", "z", "y", "c"))
    placed = (P(("y", "c"), ("x", "z")), P(), P())

    return jax.shard_map(on_device, mesh=split, in_specs=placed, out_specs=(P(("x", "z")), P()), check_vma=False)
```

```python
import functools

import jax
import jax.numpy as jnp
from jax import lax
from jax.experimental import pallas as pl
from jax.experimental.pallas import tpu as pltpu
from jax.sharding import Mesh
from jax.sharding import PartitionSpec as P


SWAP = [(0, 1), (1, 0)]
LANES = 128
BF, F32 = jnp.bfloat16, jnp.float32
HIGH = lax.Precision.HIGHEST
VMEM = pl.BlockSpec(memory_space=pltpu.VMEM)
SMEM = pl.BlockSpec(memory_space=pltpu.SMEM)


def iota(shape, dim):
    return lax.broadcasted_iota(jnp.int32, shape, dim)


def ring_by_core(n):
    pairs = []
    for k in range(n):
        pairs.append((2 * k, 2 * ((k - 1) % n)))
        pairs.append((2 * k + 1, 2 * ((k + 1) % n) + 1))
    return pairs


def turn(x_ref, out_ref, turned_ref, *, part):
    rows, width = x_ref.shape
    count, deep, _ = out_ref.shape
    cols, over = width // count, part - LANES
    low = deep - cols
    same = (iota((LANES, LANES), 0) == iota((LANES, LANES), 1)).astype(BF)
    turned_ref[...] = jnp.zeros_like(turned_ref)
    for at in range(0, width, LANES):
        block = x_ref[:, at : at + LANES]
        turned = lax.dot_general(same, block, (((1,), (1,)), ((), ())), preferred_element_type=F32)
        turned_ref[at : at + LANES, 0:rows] = turned.astype(BF)
    for k in range(count):
        out_ref[k, 0:cols, :] = turned_ref[k * cols : (k + 1) * cols, 0:LANES]
        out_ref[k, cols:deep, :] = jnp.zeros((low, LANES), BF)
        for g in range(cols // low):
            at = k * cols + g * low
            out_ref[k, cols:deep, g * over : (g + 1) * over] = turned_ref[at : at + low, LANES:part]


def prepare(x_ref, own_ref, *, occ, own):
    width = occ * own
    rows = x_ref.shape[0]
    target = iota((1, width), 1)
    source = lax.rem(target, own) * occ + lax.div(target, own)
    hot = (iota((width, width), 0) == source).astype(BF)
    moved = jnp.dot(x_ref[...], hot, preferred_element_type=F32)
    own_ref[...] = jnp.zeros_like(own_ref)
    own_ref[pl.ds(0, rows), :] = moved.astype(BF)


def joined(at_ref, own_ref, other_ref, out_ref, *, part):
    ny, deep, _ = own_ref.shape
    cols, over = out_ref.shape[0], part - LANES
    low = deep - cols
    y, c = at_ref[2], at_ref[3]
    for k in range(ny):
        step = k if k <= ny // 2 else ny // 2 - k
        near, far = (own_ref, other_ref) if step >= 0 else (other_ref, own_ref)
        source = lax.rem(y + ny + (1 - 2 * c) * step, ny)
        for at, ref in ((2 * k * part, near), ((2 * k + 1) * part, far)):
            out_ref[:, at : at + LANES] = ref[source, 0:cols, :]
            for g in range(cols // low):
                tail = ref[source, cols:deep, g * over : (g + 1) * over]
                out_ref[g * low : (g + 1) * low, at + LANES : at + part] = tail


def stack(pieces, out_ref):
    at = 0
    for piece in pieces:
        for k in range(piece.shape[0]):
            out_ref[at : at + piece.shape[1], :] = piece[k]
            at += piece.shape[1]


def transposed_groups(tiles, lane):
    a, b, c, d = tiles
    low = lane < 64
    a, c = jnp.where(low, a, pltpu.roll(c, 64, 1)), jnp.where(low, pltpu.roll(a, 64, 1), c)
    b, d = jnp.where(low, b, pltpu.roll(d, 64, 1)), jnp.where(low, pltpu.roll(b, 64, 1), d)
    even = (lane // 32) % 2 == 0
    a, b = jnp.where(even, a, pltpu.roll(b, 32, 1)), jnp.where(even, pltpu.roll(a, 96, 1), b)
    c, d = jnp.where(even, c, pltpu.roll(d, 32, 1)), jnp.where(even, pltpu.roll(c, 96, 1), d)
    return a, b, c, d


def energies(at_ref, eps_ref, virt_ref, b0_ref, b1_ref, *refs, occ, own, nx, nz, few, k, weight, pieces):
    *refs, c_ref, b_ref = refs
    if pieces:
        left_ref, sum_ref, share_ref = refs[pieces:]
        stack(refs[:pieces], left_ref)
    else:
        left_ref, before_ref, sum_ref, share_ref = refs
    half = b0_ref.shape[0]
    b_ref[pl.ds(0, half), :] = b0_ref[...]
    b_ref[pl.ds(half, half), :] = b1_ref[...]
    found = jnp.dot(b_ref[...], left_ref[...], preferred_element_type=F32)
    for t in range(c_ref.shape[0]):
        c_ref[t] = found[:, t * LANES : (t + 1) * LANES]
    lane, row = iota((8, LANES), 1), iota((8, LANES), 0)
    x, z, y, c = (at_ref[n] for n in range(4))
    vb = jnp.zeros((8, LANES), F32)
    for r in range(8):
        unit = r // few
        beside = jnp.where(c == 0, 2 * unit, 3 - 2 * unit)
        there = lax.rem(x + beside, nx) * nz + lax.rem(z + jnp.where(c == 0, k, nz - k), nz)
        vb = jnp.where(row == r, virt_ref[there * own + y * few + r % few], vb)
    va = jnp.zeros((8, LANES), F32)
    for a in range(own):
        va = jnp.where(lax.rem(lane, own) == a, virt_ref[(x * nz + z) * own + a], va)
    va = va + vb
    groups = occ // 4

    def tile(j, t):
        return c_ref[t, pl.ds(j, 8, stride=occ), :]

    share = jnp.zeros((8, LANES), F32)
    for ti in range(groups):
        la = -va
        for g in range(4):
            la = jnp.where(lax.div(lane, own) == g, eps_ref[4 * ti + g] - va, la)
        at = slice(ti * LANES, (ti + 1) * LANES)
        for tj in range(groups):
            other = transposed_groups([tile(4 * ti + g, tj) for g in range(4)], lane)
            for g in range(4):
                j = 4 * tj + g
                m = tile(j, ti)
                e = m * (2.0 * m - other[g]) / (la + eps_ref[j])
                if weight != 1.0:
                    e = e * weight
                share = share + e
                total = jnp.sum(e, axis=0, keepdims=True)
                sum_ref[j : j + 1, at] = total if pieces else total + before_ref[j : j + 1, at]
    share_ref[...] = share


def finish(at_ref, total_ref, *refs, occ, own, nx, nz, few):
    *share_refs, out_ref = refs
    width = total_ref.shape[1]
    x, z, y, c = (at_ref[n] for n in range(4))
    wide, spots = 4 * LANES, nz * own
    total = total_ref[...]
    hot = (iota((width, wide), 1) % occ == iota((width, wide), 0) // own).astype(F32)
    pairs = jnp.dot(total, hot, preferred_element_type=F32, precision=HIGH)
    pairs = jnp.where(iota((occ, wide), 1) // occ == iota((occ, wide), 0), pairs, 0.0)
    pairs = jnp.sum(pairs, axis=0, keepdims=True)
    spot = iota((width, spots), 1)
    hot = ((spot // own == z) & (spot % own == iota((width, spots), 0) % own)).astype(F32)
    left = jnp.dot(jnp.sum(total, axis=0, keepdims=True), hot, preferred_element_type=F32, precision=HIGH)
    row, spot = iota((8, spots), 0), iota((8, spots), 1)
    kept = jnp.zeros((8, spots), F32)
    for k, ref in enumerate(share_refs):
        share = jnp.sum(ref[...], axis=1, keepdims=True)
        goal = lax.rem(z + jnp.where(c == 0, k, nz - k), nz) * own + y * few + lax.rem(row, few)
        kept = kept + jnp.where(spot == goal, share, 0.0)
    unit = lax.div(row[:, 0:1], few)
    shift = jnp.where(c == 0, 2 * unit, 3 - 2 * unit)
    each = out_ref.shape[0] // nx
    for there in range(nx):
        mine = jnp.sum(jnp.where(lax.rem(x + shift, nx) == there, kept, 0.0), axis=0, keepdims=True)
        mine = mine + jnp.where(x == there, left, 0.0)
        for k in range(there * each, (there + 1) * each):
            out_ref[k, :, 0:spots] = mine
            out_ref[k, :, spots : spots + wide] = pairs


def middle(in_ref, out_ref, *, own):
    got = jnp.sum(in_ref[...], axis=0)
    nz = out_ref.shape[0]
    spots = nz * own
    for k in range(nz):
        base = (k * own) // LANES * LANES
        piece = got[:, base : base + LANES]
        turned = (LANES - (k * own - base)) % LANES
        out_ref[k, :, 0:LANES] = pltpu.roll(piece, turned, 1) if turned else piece
        out_ref[k, :, LANES:] = got[:, spots:]


def last(in_ref, virt_ref, pair_ref, *, occ, own):
    got = jnp.sum(in_ref[...], axis=0)
    virt_ref[...] = got[:, 0:own]
    row = got[:, LANES:]
    wide = row.shape[1]
    n, j = iota((occ, wide), 1), iota((occ, wide), 0)
    m, i = iota((wide, occ), 0), iota((wide, occ), 1)
    one = jnp.dot(jnp.where(n // occ == j, row, 0.0), (m % occ == i).astype(F32), preferred_element_type=F32, precision=HIGH)
    two = jnp.dot(jnp.where(n % occ == j, jnp.where(n < occ * occ, row, 0.0), 0.0), (m // occ == i).astype(F32), preferred_element_type=F32, precision=HIGH)
    pair_ref[...] = one + two


def shape(*dims, kind=F32):
    return jax.ShapeDtypeStruct(dims, kind)


def on_device(three_index, eps_occ, eps_virt):
    occ = eps_occ.shape[0]
    rows, width = three_index.shape
    own = width // occ
    nx, nz, ny = lax.axis_size("x"), lax.axis_size("z"), lax.axis_size("y")
    parts = 2 * ny
    x, z, y, c = (lax.axis_index(k) for k in ("x", "z", "y", "c"))
    few = own // ny
    cols = few * occ
    part = -(-rows // 8) * 8
    steps = nz // 2
    place = jnp.stack([x, z, y, c]).astype(jnp.int32)

    def kernel(f, out, spaces, cost=0, scratch=(), **static):
        several = isinstance(out, list)
        return pl.pallas_call(
            functools.partial(f, **static),
            out_shape=out,
            in_specs=spaces,
            out_specs=[VMEM] * len(out) if several else VMEM,
            scratch_shapes=scratch,
            compiler_params=pltpu.CompilerParams(vmem_limit_bytes=16 << 20),
            cost_estimate=pl.CostEstimate(flops=cost, bytes_accessed=1 << 20, transcendentals=0),
        )

    low = 16
    scratch = [pltpu.VMEM((width, 2 * LANES), BF)]
    turned = kernel(turn, shape(ny, cols + low, LANES, kind=BF), [VMEM], scratch=scratch, part=part)(three_index)
    tiles = lax.all_to_all(turned, "y", split_axis=0, concat_axis=0, tiled=True)
    theirs = lax.ppermute(tiles, "c", SWAP)
    unit = kernel(joined, shape(cols, parts * part, kind=BF), [SMEM] + [VMEM] * 2, part=part)(place, tiles, theirs)

    mine = kernel(prepare, shape(part, width, kind=BF), [VMEM], occ=occ, own=own)(three_index)
    both = jnp.stack([mine, lax.ppermute(mine, "c", SWAP)])
    arrived, moving = [], both
    for _ in range(ny // 2):
        moving = lax.ppermute(moving, ("y", "c"), ring_by_core(ny))
        arrived.append(moving)
    collected = jnp.concatenate(arrived[:-1])
    outer = lax.ppermute(collected, "c", SWAP)

    def beside(n):
        return [(2 * m + core, 2 * ((m - 2 * n + core * (4 * n - 3)) % nx) + core) for m in range(nx) for core in range(2)]

    one, two = (lax.ppermute(unit, ("x", "c"), beside(n)) for n in range(2))
    total, shares = None, []
    for k in range(steps + 1):
        if k:
            one = lax.ppermute(one, ("z", "c"), ring_by_core(nz))
            two = lax.ppermute(two, ("z", "c"), ring_by_core(nz))
        given = (left, total) if k else (both, *arrived, outer)
        sizes = [shape(occ, width), shape(8, LANES)]
        call = kernel(
            energies,
            sizes if k else [shape(parts * part, width, kind=BF), *sizes],
            [SMEM] * 3 + [VMEM] * (2 + len(given)),
            cost=4 * cols * width * parts * part,
            scratch=[
                pltpu.VMEM((width // LANES, 2 * cols, LANES), F32),
                pltpu.VMEM((2 * cols, parts * part), BF),
            ],
            occ=occ, own=own, nx=nx, nz=nz, few=few, k=k,
            weight=0.5 if k in (0, steps) else 1.0,
            pieces=0 if k else len(given),
        )
        results = call(place, eps_occ, eps_virt, one, two, *given)
        if k == 0:
            left, *results = results
        total, share = results
        shares.append(share)

    wide = nz * own + 4 * LANES
    slots = kernel(
        finish, shape(nx * parts, 1, wide), [SMEM] + [VMEM] * (2 + steps), occ=occ, own=own, nx=nx, nz=nz, few=few
    )(place, total, *shares)
    slots = lax.all_to_all(slots, ("x", "y", "c"), split_axis=0, concat_axis=0, tiled=True)
    slots = kernel(middle, shape(nz, 1, 5 * LANES), [VMEM], own=own)(slots)
    slots = lax.all_to_all(slots, "z", split_axis=0, concat_axis=0, tiled=True)
    virt, pairs = kernel(last, [shape(1, own), shape(occ, occ)], [VMEM], occ=occ, own=own)(slots)
    return virt.reshape(own), pairs


def solution(mesh):
    split = Mesh(mesh.devices.reshape(4, 8, mesh.shape["aux"] // 2, 2), ("x", "z", "y", "c"))
    placed = (P(("y", "c"), ("x", "z")), P(), P())

    return jax.shard_map(on_device, mesh=split, in_specs=placed, out_specs=(P(("x", "z")), P()), check_vma=False)
```
